256 devices in a mesh: dp: 16 (over y, x_lo, core), seq: 16 (over x_hi, z).
Axes of the slice: x: 4 (x_hi: 2, x_lo: 2; x = x_hi * 2 + x_lo), y: 4, z: 8, core: 2. Of those that a mesh axis runs over, the one named last changes fastest.
Arguments:
- queries: bfloat16 [65536, 1664], P(('dp', 'seq')), parts along dimension 0, may hold values from -6 to 6
- key_rows: bfloat16 [65536, 1664], P(('dp', 'seq')), parts along dimension 0, may hold values from -6 to 6
- value_rows: bfloat16 [65536, 1664], P(('dp', 'seq')), parts along dimension 0, may hold values from -6 to 6
Outputs:
- merged_tokens: bfloat16 [16384, 6656], P('dp', 'seq'), parts along dimension 0
The draws below stay inside these ranges and needn't reach their ends.
There are 16 independent parts, one for each index of `dp`. The reference program is written for one: setup_inputs(seed, part) draws one part's arguments, and reference() takes and returns one part's arrays. A program takes and returns all parts, laid end to end along the dimension named above; each array names one. Nothing has to cross between parts.
All inputs are finite; a program needn't handle non-finite values.
Results may differ from the reference program's by a relative error of at most 0.005.
Values may be sent and summed in bfloat16 or wider, within the bound.
A program may use at most 128 MiB of HBM per device.

```python
import math
import jax
import jax.numpy as jnp
from jax import lax

HEADS = 13
HEAD_DIM = 128
GRID_W = 64
TOKENS = 4096
CH = 1664


def draw_pair(key):
    width = HEADS * HEAD_DIM
    query_key = jax.random.fold_in(key, 11)
    other_key = jax.random.fold_in(key, 12)
    queries = 1.6 * jax.random.truncated_normal(query_key, -3.75, 3.75, (TOKENS, width), jnp.float32)
    key_rows = 1.6 * jax.random.truncated_normal(other_key, -3.75, 3.75, (TOKENS, width), jnp.float32)
    return (queries, key_rows)


def draw_queries(key, part):
    return draw_pair(key)[0].astype(jnp.bfloat16)


def draw_key_rows(key, part):
    return draw_pair(key)[1].astype(jnp.bfloat16)


def block_levels(stream_key, shape, split, least, top_value):
    loudness, own = 1.0, jax.random.fold_in(stream_key, 6)
    for axis_at, blocks in split:
        heights = jnp.exp(jax.random.uniform(jax.random.fold_in(own, axis_at), (blocks,), jnp.float32, least / len(split), top_value / len(split)))
        loudness = loudness * jnp.repeat(heights, shape[axis_at] // blocks).reshape([-1 if axis == axis_at else 1 for axis in range(len(shape))])
    return loudness


def centred(own_key, extent, spread, limit, pieces=(), dtype=jnp.bfloat16):
    gain = block_levels(own_key, extent, pieces, -0.22, 0.18) if pieces else 1.0
    drawn = jax.random.normal(own_key, extent, jnp.float32) * spread * gain
    return jnp.minimum(jnp.maximum(drawn, -limit), limit).astype(dtype)


def setup_inputs(seed: int = 0, part: int = 0) -> dict:
    keys = jax.random.split(jax.random.key(seed), 4)
    own_keys = jax.random.split(jax.random.fold_in(keys[3], part), 4)
    queries = draw_queries(jax.random.fold_in(jax.random.fold_in(keys[3], part), 71), part)
    key_rows = draw_key_rows(jax.random.fold_in(jax.random.fold_in(keys[3], part), 71), part)
    value_rows = centred(own_keys[2], (TOKENS, CH), 1.0, 6.0, ((0, 16),))
    return {"queries": queries, "key_rows": key_rows, "value_rows": value_rows}


def one_head(query_head, key_head, value_head):
    total_rows = query_head.shape[0]
    block_rows = math.gcd(total_rows, 512)
    score_scale = 1.0 / math.sqrt(HEAD_DIM)
    blocks = query_head.reshape(total_rows // block_rows, block_rows, HEAD_DIM)

    def attend(query_block):
        scores = jnp.dot(query_block, key_head.T, preferred_element_type=jnp.float32) * score_scale
        row_max = lax.optimization_barrier(jnp.max(scores, axis=-1, keepdims=True))
        weights = jnp.exp(scores - row_max)
        totals = lax.optimization_barrier(jnp.sum(weights, axis=-1, keepdims=True))
        weighted = jnp.dot(weights.astype(jnp.bfloat16), value_head, preferred_element_type=jnp.float32)
        return (weighted / totals).astype(jnp.bfloat16)
    return lax.map(attend, blocks).reshape(total_rows, HEAD_DIM)

def reference(queries, key_rows, value_rows):
    tokens = queries.shape[0]
    query_heads = queries.reshape(tokens, HEADS, HEAD_DIM).transpose(1, 0, 2)
    key_heads = key_rows.reshape(tokens, HEADS, HEAD_DIM).transpose(1, 0, 2)
    value_heads = value_rows.reshape(tokens, HEADS, HEAD_DIM).transpose(1, 0, 2)
    attended = lax.map(lambda triple: one_head(triple[0], triple[1], triple[2]), (query_heads, key_heads, value_heads))
    attended = attended.transpose(1, 0, 2).reshape(tokens, HEADS * HEAD_DIM)
    grid_rows = tokens // GRID_W
    shuffled = attended.reshape(grid_rows // 2, 2, GRID_W // 2, 2, HEADS * HEAD_DIM).transpose(0, 2, 1, 3, 4)
    return shuffled.reshape(grid_rows // 2 * (GRID_W // 2), 4 * HEADS * HEAD_DIM)
```

```python
import functools
import math

import jax
import jax.numpy as jnp
from jax import lax
from jax.experimental import pallas as pl
from jax.experimental.pallas import tpu as pltpu
from jax.sharding import PartitionSpec as P

HEAD_DIM = 128
MESH = pl.DeviceIdType.MESH
HEAD_AT = (
    (6, -1, 0, -1, 7, 10, -1, 3, 8, 11, 1, 4, 9, 12, 2, 5),
    (6, 10, 0, 3, 7, 11, 1, 4, 8, 12, -1, 5, 9, -1, 2, -1),
)
STEPS = ((0, 1), (1, 7), (0, 7), (1, 1), (0, 2), (1, 6), (0, 6), (1, 2),
         (0, 3), (1, 5), (0, 5), (1, 3), (0, 4), (1, 4), (1, 0))


def pick(table, index):
    value = jnp.int32(table[0])
    for place in range(1, len(table)):
        value = jnp.where(index == place, jnp.int32(table[place]), value)
    return value


def exchange(q_hbm, k_hbm, v_hbm, out_ref, kbuf, vbuf, qbuf, sbuf, pbuf, obuf, stage, merged,
             send_sem, k_sem, v_sem, q_sem, out_send, out_recv):
    me = lax.axis_index("seq")
    core = lax.rem(lax.axis_index("dp"), 2)
    rows = q_hbm.shape[0]
    peers = 16
    x_hi, z = lax.div(me, 8), lax.rem(me, 8)

    def place(dx, dz):
        return lax.rem(x_hi + dx, 2) * 8 + lax.rem(z + dz, 8)

    def head_at(where):
        return jnp.where(core == 0, pick(HEAD_AT[0], where), pick(HEAD_AT[1], where))

    my_head = head_at(me)
    owner = my_head >= 0

    barrier = pltpu.get_barrier_semaphore()
    for other in range(1, peers):
        pl.semaphore_signal(barrier, inc=1, device_id={"seq": lax.rem(me + other, peers)}, device_id_type=MESH)
    vbuf[:, HEAD_DIM:] = jnp.ones((peers * rows, HEAD_DIM), jnp.bfloat16)
    pl.semaphore_wait(barrier, peers - 1)

    targets = [place(dx, dz) for dx, dz in STEPS]
    heads = [head_at(target) for target in targets]

    def outgoing(kind, step):
        src, dst = ((k_hbm, kbuf), (v_hbm, vbuf), (q_hbm, qbuf))[kind]
        columns = pl.ds(pl.multiple_of(heads[step] * HEAD_DIM, HEAD_DIM), HEAD_DIM)
        mine = pl.ds(pl.multiple_of(me * rows, rows), rows)
        sem = (k_sem.at[0], v_sem.at[0], q_sem.at[step])[kind]
        return pltpu.make_async_remote_copy(
            src_ref=src.at[:, columns],
            dst_ref=dst.at[mine, pl.ds(0, HEAD_DIM)],
            send_sem=send_sem.at[kind, step],
            recv_sem=sem,
            device_id={"seq": targets[step]},
            device_id_type=MESH,
        )

    def local(kind):
        src, dst = ((k_hbm, kbuf), (v_hbm, vbuf), (q_hbm, qbuf))[kind]
        columns = pl.ds(pl.multiple_of(my_head * HEAD_DIM, HEAD_DIM), HEAD_DIM)
        mine = pl.ds(pl.multiple_of(me * rows, rows), rows)
        sem = (k_sem.at[0], v_sem.at[0], q_sem.at[peers - 1])[kind]
        return pltpu.make_async_copy(src.at[:, columns], dst.at[mine, pl.ds(0, HEAD_DIM)], sem)

    for kind in range(3):
        @pl.when(owner)
        def _():
            local(kind).start()
        for step in range(peers - 1):
            @pl.when(heads[step] >= 0)
            def _():
                outgoing(kind, step).start()

    low = lax.div(my_head * HEAD_DIM, 416)
    high = lax.div(my_head * HEAD_DIM + HEAD_DIM - 1, 416)
    scale = math.log2(math.e) / math.sqrt(HEAD_DIM)

    def out_copy(source, kind, group, wide):
        return pltpu.make_async_remote_copy(
            src_ref=stage.at[source, kind],
            dst_ref=merged.at[my_head - 3 * group, pl.ds(pl.multiple_of(source * 64, 64), 64)],
            send_sem=out_send.at[wide],
            recv_sem=out_recv.at[0],
            device_id={"seq": 4 * kind + group},
            device_id_type=MESH,
        )

    def send_out(source):
        for kind in range(4):
            out_copy(source, kind, low, 0).start()

        @pl.when(high != low)
        def _():
            for kind in range(4):
                out_copy(source, kind, high, 1).start()

    def source_of(turn):
        dx, dz = jnp.int32(0), jnp.int32(0)
        for step, (sx, sz) in enumerate(STEPS):
            dx = jnp.where(turn == step + 1, sx, dx)
            dz = jnp.where(turn == step + 1, (8 - sz) % 8, dz)
        return place(dx, dz)

    @pl.when(owner)
    def _():
        pltpu.make_async_copy(kbuf, kbuf, k_sem.at[0]).wait()
        pltpu.make_async_copy(vbuf.at[:, pl.ds(0, HEAD_DIM)], vbuf.at[:, pl.ds(0, HEAD_DIM)], v_sem.at[0]).wait()

        def turn_body(turn, carry):
            source = source_of(turn)
            span = pl.ds(pl.multiple_of(source * rows, rows), rows)
            sem = q_sem.at[lax.rem(turn + peers - 1, peers)]
            pltpu.make_async_copy(qbuf.at[span], qbuf.at[span], sem).wait()
            query = qbuf[span, :]
            top = None
            for part in range(8):
                cols = pl.ds(part * 512, 512)
                scores = lax.dot_general(query, kbuf[cols, :], (((1,), (1,)), ((), ())),
                                         preferred_element_type=jnp.float32)
                sbuf[:, cols] = scores
                for tile in range(4):
                    piece = scores[:, tile * 128:(tile + 1) * 128]
                    top = piece if top is None else jnp.maximum(top, piece)
            peak = jnp.max(top, axis=1, keepdims=True) * scale
            for part in range(8):
                cols = pl.ds(part * 512, 512)
                pbuf[:, cols] = jnp.exp2(sbuf[:, cols] * scale - peak).astype(jnp.bfloat16)
            both = jnp.dot(pbuf[...], vbuf[...], preferred_element_type=jnp.float32)
            obuf[...] = both[:, :HEAD_DIM] / both[:, HEAD_DIM:]
            for a in range(2):
                for b in range(2):
                    for half in range(2):
                        picked = obuf[pl.ds(128 * half + 64 * a + b, 32, stride=2), :]
                        stage[source, 2 * a + b, pl.ds(32 * half, 32), :] = picked.astype(jnp.bfloat16)
            send_out(source)
            return carry

        lax.fori_loop(0, peers, turn_body, 0)

    pltpu.make_async_copy(merged, merged, out_recv.at[0]).wait()
    group = lax.rem(z, 4)
    for shift in range(4):
        @pl.when(group == shift)
        def _():
            def lay(chunk, carry):
                span = pl.ds(pl.multiple_of(chunk * 128, 128), 128)
                wide = jnp.concatenate([merged[slot, span, :] for slot in range(4)], axis=1)
                out_ref[span, :] = wide[:, 32 * shift:32 * shift + 416]
                return carry
            lax.fori_loop(0, 8, lay, 0)

    for kind in range(3):
        for step in range(peers - 1):
            @pl.when(heads[step] >= 0)
            def _():
                outgoing(kind, step).wait_send()

    @pl.when(owner)
    def _():
        pltpu.make_async_copy(stage, stage, out_send.at[0]).wait()

        @pl.when(high != low)
        def _():
            pltpu.make_async_copy(stage, stage, out_send.at[1]).wait()


def on_device(queries, key_rows, value_rows):
    rows = queries.shape[0]
    total = rows * 16
    any_spec = pl.BlockSpec(memory_space=pl.ANY)
    return pl.pallas_call(
        exchange,
        out_shape=jax.ShapeDtypeStruct((total // 4, 416), jnp.bfloat16),
        in_specs=[any_spec] * 3,
        out_specs=pl.BlockSpec(memory_space=pltpu.VMEM),
        scratch_shapes=[
            pltpu.VMEM((total, HEAD_DIM), jnp.bfloat16),
            pltpu.VMEM((total, 2 * HEAD_DIM), jnp.bfloat16),
            pltpu.VMEM((total, HEAD_DIM), jnp.bfloat16),
            pltpu.VMEM((rows, total), jnp.float32),
            pltpu.VMEM((rows, total), jnp.bfloat16),
            pltpu.VMEM((rows, HEAD_DIM), jnp.float32),
            pltpu.VMEM((16, 4, rows // 4, HEAD_DIM), jnp.bfloat16),
            pltpu.VMEM((4, total // 4, HEAD_DIM), jnp.bfloat16),
            pltpu.SemaphoreType.DMA((3, 15)),
            pltpu.SemaphoreType.DMA((1,)),
            pltpu.SemaphoreType.DMA((1,)),
            pltpu.SemaphoreType.DMA((16,)),
            pltpu.SemaphoreType.DMA((2,)),
            pltpu.SemaphoreType.DMA((1,)),
        ],
        compiler_params=pltpu.CompilerParams(collective_id=0, has_side_effects=True, vmem_limit_bytes=56 * 1024 * 1024),
    )(queries, key_rows, value_rows)


def solution(mesh):
    placed = (P(("dp", "seq"), None), P(("dp", "seq"), None), P(("dp", "seq"), None))
    return jax.shard_map(
        on_device, mesh=mesh, in_specs=placed, out_specs=P("dp", "seq"), check_vma=False
    )
```

```python
import functools
import math

import jax
import jax.numpy as jnp
from jax import lax
from jax.experimental import pallas as pl
from jax.experimental.pallas import tpu as pltpu
from jax.sharding import PartitionSpec as P

HEAD_DIM = 128
CHUNK = 512
MESH = pl.DeviceIdType.MESH
HEAD_AT = (
    (6, -1, 0, -1, 7, 10, -1, 3, 8, 11, 1, 4, 9, 12, 2, 5),
    (6, 10, 0, 3, 7, 11, 1, 4, 8, 12, -1, 5, 9, -1, 2, -1),
)
STEPS = ((0, 1), (1, 7), (0, 7), (1, 1), (0, 2), (1, 6), (0, 6), (1, 2),
         (0, 3), (1, 5), (0, 5), (1, 3), (0, 4), (1, 4), (1, 0))


def pick(table, index):
    value = jnp.int32(table[0])
    for place in range(1, len(table)):
        value = jnp.where(index == place, jnp.int32(table[place]), value)
    return value


def dot(a, b, dims):
    return lax.dot_general(a, b, (dims, ((), ())), preferred_element_type=jnp.float32)


def exchange(q_hbm, k_hbm, v_hbm, out_ref, kbuf, vbuf, vflip, qbuf, sbuf0, sbuf1, pbuf, obuf, stage, merged,
             send_sem, k_sem, v_sem, q_sem, out_send, out_recv):
    me = lax.axis_index("seq")
    core = lax.rem(lax.axis_index("dp"), 2)
    rows = q_hbm.shape[0]
    peers = 16
    tokens = rows * peers
    parts = tokens // CHUNK
    x_hi, z = lax.div(me, 8), lax.rem(me, 8)

    def place(dx, dz):
        return lax.rem(x_hi + dx, 2) * 8 + lax.rem(z + dz, 8)

    def head_at(where):
        return jnp.where(core == 0, pick(HEAD_AT[0], where), pick(HEAD_AT[1], where))

    my_head = head_at(me)
    owner = my_head >= 0

    barrier = pltpu.get_barrier_semaphore()
    for other in range(1, peers):
        pl.semaphore_signal(barrier, inc=1, device_id={"seq": lax.rem(me + other, peers)}, device_id_type=MESH)

    targets = [place(dx, dz) for dx, dz in STEPS]
    heads = [head_at(target) for target in targets]
    pl.semaphore_wait(barrier, peers - 1)

    def lanes_of(head):
        return pl.ds(pl.multiple_of(head * HEAD_DIM, HEAD_DIM), HEAD_DIM)

    def rows_of(source):
        return pl.ds(pl.multiple_of(source * rows, rows), rows)

    def outgoing(kind, step):
        src, dst = ((k_hbm, kbuf), (v_hbm, vbuf), (q_hbm, qbuf))[kind]
        sem = (k_sem.at[0], v_sem.at[step + 1], q_sem.at[step + 1])[kind]
        return pltpu.make_async_remote_copy(
            src_ref=src.at[:, lanes_of(heads[step])],
            dst_ref=dst.at[rows_of(me)],
            send_sem=send_sem.at[kind, step],
            recv_sem=sem,
            device_id={"seq": targets[step]},
            device_id_type=MESH,
        )

    def local(kind):
        src, dst = ((k_hbm, kbuf), (v_hbm, vbuf), (q_hbm, qbuf))[kind]
        sem = (k_sem.at[0], v_sem.at[0], q_sem.at[0])[kind]
        return pltpu.make_async_copy(src.at[:, lanes_of(my_head)], dst.at[rows_of(me)], sem)

    for kind in range(3):
        @pl.when(owner)
        def _():
            local(kind).start()
        for step in range(peers - 1):
            @pl.when(heads[step] >= 0)
            def _():
                outgoing(kind, step).start()

    first = my_head * 4
    low, high = lax.div(first, 13), lax.div(first + 3, 13)
    scale = math.log2(math.e) / math.sqrt(HEAD_DIM)

    def out_copy(source, kind, group, unit, units):
        base = (my_head - 3 * group) * (tokens // 4) + source * (rows // 4) + 16 * unit
        return pltpu.make_async_remote_copy(
            src_ref=stage.at[source, kind, pl.ds(16 * unit, 16 * units)],
            dst_ref=merged.at[pl.ds(pl.multiple_of(base, 16), 16 * units)],
            send_sem=out_send.at[0],
            recv_sem=out_recv.at[0],
            device_id={"seq": 4 * kind + group},
            device_id_type=MESH,
        )

    def send_out(source):
        @pl.when(high == low)
        def _():
            for kind in range(4):
                out_copy(source, kind, low, 0, 4).start()

        @pl.when(high != low)
        def _():
            for kind in range(4):
                for unit in range(4):
                    out_copy(source, kind, lax.div(first + unit, 13), unit, 1).start()

    def source_of(turn):
        dx, dz = jnp.int32(0), jnp.int32(0)
        for step, (sx, sz) in enumerate(STEPS):
            dx = jnp.where(turn == step + 1, sx, dx)
            dz = jnp.where(turn == step + 1, (8 - sz) % 8, dz)
        return place(dx, dz)

    def fold(x, op):
        return op(x.reshape(x.shape[0] // 8, 8, x.shape[1]), axis=0)

    def load_query(turn):
        span = rows_of(source_of(turn))
        pltpu.make_async_copy(qbuf.at[span], qbuf.at[span], q_sem.at[turn]).wait()
        return qbuf[span, :]

    def score_part(query, scores, part, top):
        span = pl.ds(part * CHUNK, CHUNK)
        piece = dot(kbuf[span, :], query, ((1,), (1,)))
        scores[span, :] = piece
        return jnp.maximum(top, fold(piece, jnp.max))

    def weight_part(scores, part, peak, total):
        span = pl.ds(part * CHUNK, CHUNK)
        weights = jnp.exp2(scores[span, :] * scale - peak)
        pbuf[span, :] = weights.astype(jnp.bfloat16)
        return total + fold(weights, jnp.sum)

    def peak_of(top):
        return jnp.max(top, axis=0, keepdims=True) * scale

    def finish(turn, total):
        source = source_of(turn)
        result = dot(vflip[...], pbuf[...], ((1,), (0,)))
        obuf[...] = (result / jnp.sum(total, axis=0, keepdims=True)).T
        for kind in range(4):
            picked = [
                obuf[pl.ds(128 * (g // 2) + 32 * (g % 2) + 64 * (kind // 2) + kind % 2, 16, stride=2), :]
                for g in range(4)
            ]
            for unit in range(4):
                stage[source, kind, pl.ds(16 * unit, 16), :] = jnp.concatenate(
                    [piece[:, 32 * unit:32 * unit + 32] for piece in picked], axis=1
                ).astype(jnp.bfloat16)
        send_out(source)

    none = jnp.full((8, rows), -jnp.inf, jnp.float32)
    zero = jnp.zeros((8, rows), jnp.float32)

    def turn_both(turn, peak, now, after):
        query = load_query(turn + 1)
        top, total = none, zero
        for part in range(parts):
            top = score_part(query, after, part, top)
            total = weight_part(now, part, peak, total)
        finish(turn, total)
        return peak_of(top)

    def turn_last(turn, peak, now):
        total = zero
        for part in range(parts):
            total = weight_part(now, part, peak, total)
        finish(turn, total)

    @pl.when(owner)
    def _():
        pltpu.make_async_copy(kbuf, kbuf, k_sem.at[0]).wait()

        def flip(turn, carry):
            span = rows_of(source_of(turn))
            pltpu.make_async_copy(vbuf.at[span], vbuf.at[span], v_sem.at[turn]).wait()
            vflip[:, span] = vbuf[span, :].T
            return carry

        lax.fori_loop(0, peers, flip, 0)
        query = load_query(0)
        top = none
        for part in range(parts):
            top = score_part(query, sbuf0, part, top)

        def pair(two, peak):
            peak = turn_both(2 * two, peak, sbuf0, sbuf1)
            return turn_both(2 * two + 1, peak, sbuf1, sbuf0)

        peak = lax.fori_loop(0, peers // 2 - 1, pair, peak_of(top))
        peak = turn_both(jnp.int32(peers - 2), peak, sbuf0, sbuf1)
        turn_last(jnp.int32(peers - 1), peak, sbuf1)

    held = merged.at[pl.ds(0, tokens * 416 // 512)]
    pltpu.make_async_copy(held, held, out_recv.at[0]).wait()
    group = lax.rem(z, 4)
    starts = []
    for unit in range(13):
        where = group + unit
        starts.append(lax.div(where, 4) * (tokens // 4) + lax.rem(where, 4) * 16)

    def lay(source, carry):
        for g in range(4):
            units = [
                merged[pl.ds(pl.multiple_of(start + source * (rows // 4), 16), 16), 32 * g:32 * g + 32]
                for start in starts
            ]
            out_ref[pl.ds(pl.multiple_of(source * (rows // 4) + 16 * g, 16), 16), :] = jnp.concatenate(units, axis=1)
        return carry

    lax.fori_loop(0, peers, lay, 0)

    for kind in range(3):
        for step in range(peers - 1):
            @pl.when(heads[step] >= 0)
            def _():
                outgoing(kind, step).wait_send()

    @pl.when(owner)
    def _():
        pltpu.make_async_copy(stage, stage, out_send.at[0]).wait()


def on_device(queries, key_rows, value_rows):
    rows = queries.shape[0]
    total = rows * 16
    any_spec = pl.BlockSpec(memory_space=pl.ANY)
    return pl.pallas_call(
        exchange,
        out_shape=jax.ShapeDtypeStruct((total // 4, 416), jnp.bfloat16),
        in_specs=[any_spec] * 3,
        out_specs=pl.BlockSpec(memory_space=pltpu.VMEM),
        scratch_shapes=[
            pltpu.VMEM((total, HEAD_DIM), jnp.bfloat16),
            pltpu.VMEM((total, HEAD_DIM), jnp.bfloat16),
            pltpu.VMEM((HEAD_DIM, total), jnp.bfloat16),
            pltpu.VMEM((total, HEAD_DIM), jnp.bfloat16),
            pltpu.VMEM((total, rows), jnp.float32),
            pltpu.VMEM((total, rows), jnp.float32),
            pltpu.VMEM((total, rows), jnp.bfloat16),
            pltpu.VMEM((rows, HEAD_DIM), jnp.float32),
            pltpu.VMEM((16, 4, rows // 4, HEAD_DIM), jnp.bfloat16),
            pltpu.VMEM((total, HEAD_DIM), jnp.bfloat16),
            pltpu.SemaphoreType.DMA((3, 15)),
            pltpu.SemaphoreType.DMA((1,)),
            pltpu.SemaphoreType.DMA((16,)),
            pltpu.SemaphoreType.DMA((16,)),
            pltpu.SemaphoreType.DMA((1,)),
            pltpu.SemaphoreType.DMA((1,)),
        ],
        compiler_params=pltpu.CompilerParams(collective_id=0, has_side_effects=True, vmem_limit_bytes=56 * 1024 * 1024),
    )(queries, key_rows, value_rows)


def solution(mesh):
    placed = (P(("dp", "seq"), None), P(("dp", "seq"), None), P(("dp", "seq"), None))
    return jax.shard_map(
        on_device, mesh=mesh, in_specs=placed, out_specs=P("dp", "seq"), check_vma=False
    )
```

```python
import functools
import math

import jax
import jax.numpy as jnp
from jax import lax
from jax.experimental import pallas as pl
from jax.experimental.pallas import tpu as pltpu
from jax.sharding import PartitionSpec as P

HEAD_DIM = 128
CHUNK = 512
VMEM_LIMIT = 60 * 1024 * 1024
MESH = pl.DeviceIdType.MESH
HEAD_AT = (
    (6, 10, 0, 3, 7, 11, 1, 4, 8, 12, -1, 5, 9, -1, 2, -1),
    (6, -1, 0, -1, 7, 10, -1, 3, 8, 11, 1, 4, 9, 12, 2, 5),
)
STEPS = ((0, 1), (1, 7), (0, 7), (1, 1), (0, 2), (1, 6), (0, 6), (1, 2),
         (0, 3), (1, 5), (0, 5), (1, 3), (0, 4), (1, 4), (1, 0))
PAIRS = ((0, 0), (1, 0), (0, 1), (1, 3), (0, 3), (1, 1), (0, 2), (1, 2))


def pick(table, index):
    value = jnp.int32(table[0])
    for place in range(1, len(table)):
        value = jnp.where(index == place, jnp.int32(table[place]), value)
    return value


def dot(a, b, dims):
    return lax.dot_general(a, b, (dims, ((), ())), preferred_element_type=jnp.float32)


def exchange(q_hbm, k_hbm, v_hbm, out_ref, kbuf, vbuf, vflip, qbuf, qwide, sbuf0, sbuf1, pbuf, stage,
             send_sem, k_sem, v_sem, q_sem, out_send, out_recv):
    me = lax.axis_index("seq")
    core = lax.rem(lax.axis_index("dp"), 2)
    rows = q_hbm.shape[0]
    peers = 16
    tokens = rows * peers
    parts = tokens // CHUNK
    x_hi, z = lax.div(me, 8), lax.rem(me, 8)

    def place(dx, dz):
        return lax.rem(x_hi + dx, 2) * 8 + lax.rem(z + dz, 8)

    def head_at(where):
        return jnp.where(core == 0, pick(HEAD_AT[0], where), pick(HEAD_AT[1], where))

    my_head = head_at(me)
    owner = my_head >= 0

    barrier = pltpu.get_barrier_semaphore()
    for other in range(1, peers):
        pl.semaphore_signal(barrier, inc=1, device_id={"seq": lax.rem(me + other, peers)}, device_id_type=MESH)

    targets = [place(dx, dz) for dx, dz in STEPS]
    heads = [head_at(target) for target in targets]
    pl.semaphore_wait(barrier, peers - 1)

    def lanes_of(head):
        return pl.ds(pl.multiple_of(head * HEAD_DIM, HEAD_DIM), HEAD_DIM)

    def rows_of(source):
        return pl.ds(pl.multiple_of(source * rows, rows), rows)

    def outgoing(kind, step):
        src, dst = ((k_hbm, kbuf), (v_hbm, vbuf), (q_hbm, qbuf))[kind]
        sem = (k_sem.at[0], v_sem.at[me], q_sem.at[me])[kind]
        return pltpu.make_async_remote_copy(
            src_ref=src.at[:, lanes_of(heads[step])],
            dst_ref=dst.at[rows_of(me)],
            send_sem=send_sem.at[kind, step],
            recv_sem=sem,
            device_id={"seq": targets[step]},
            device_id_type=MESH,
        )

    def local(kind):
        src, dst = ((k_hbm, kbuf), (v_hbm, vbuf), (q_hbm, qbuf))[kind]
        sem = (k_sem.at[0], v_sem.at[me], q_sem.at[me])[kind]
        return pltpu.make_async_copy(src.at[:, lanes_of(my_head)], dst.at[rows_of(me)], sem)

    for kind in range(3):
        @pl.when(owner)
        def _():
            local(kind).start()
        for step in range(peers - 1):
            @pl.when(heads[step] >= 0)
            def _():
                outgoing(kind, step).start()

    first = my_head * 4
    low, high = lax.div(first, 13), lax.div(first + 3, 13)
    scale = math.log2(math.e) / math.sqrt(HEAD_DIM)

    def out_copy(pair, kind, group, unit, units):
        row = pl.multiple_of((first + unit - 13 * group) * 32, 32)
        return pltpu.make_async_remote_copy(
            src_ref=stage.at[pair, kind, pl.ds(32 * unit, 32 * units)],
            dst_ref=out_ref.at[pl.ds(row, 32 * units), pl.ds(pl.multiple_of(pair * 128, 128), 128)],
            send_sem=out_send.at[0],
            recv_sem=out_recv.at[0],
            device_id={"seq": 4 * kind + group},
            device_id_type=MESH,
        )

    def send_out(pair, kinds):
        @pl.when(high == low)
        def _():
            for kind in kinds:
                out_copy(pair, kind, low, 0, 4).start()

        @pl.when(high != low)
        def _():
            for kind in kinds:
                for unit in range(4):
                    out_copy(pair, kind, lax.div(first + unit, 13), unit, 1).start()

    def pair_of(turn):
        dx, dp = jnp.int32(0), jnp.int32(0)
        for at, (sx, sp) in enumerate(PAIRS):
            dx = jnp.where(turn == at, sx, dx)
            dp = jnp.where(turn == at, sp, dp)
        return lax.rem(x_hi + dx, 2) * 4 + lax.rem(lax.div(z, 2) + dp, 4)

    def fold(x, op):
        return op(x.reshape(x.shape[0] // 8, 8, x.shape[1]), axis=0)

    def take_pair(pair):
        for side in range(2):
            source = 2 * pair + side
            span = rows_of(source)
            pltpu.make_async_copy(qbuf.at[span], qbuf.at[span], q_sem.at[source]).wait()
            qwide[pl.ds(side * rows, rows), :] = qbuf[span, :].astype(jnp.float32)

    def load_query(a):
        picked = [
            qwide[pl.ds(rows * side + 128 * half + 64 * a + b, 32, stride=2), :]
            for b in range(2) for side in range(2) for half in range(2)
        ]
        return jnp.concatenate(picked, axis=0).astype(jnp.bfloat16)

    def score_part(query, scores, part, top):
        span = pl.ds(part * CHUNK, CHUNK)
        piece = dot(kbuf[span, :], query, ((1,), (1,)))
        scores[span, :] = piece
        return jnp.maximum(top, fold(piece, jnp.max))

    def weight_part(scores, part, peak, total):
        span = pl.ds(part * CHUNK, CHUNK)
        weights = jnp.exp2(scores[span, :] * scale - peak)
        pbuf[span, :] = weights.astype(jnp.bfloat16)
        return total + fold(weights, jnp.sum)

    def peak_of(top):
        return jnp.max(top, axis=0, keepdims=True) * scale

    def finish(pair, a, total):
        result = dot(vflip[...], pbuf[...], ((1,), (0,)))
        result = (result / jnp.sum(total, axis=0, keepdims=True)).astype(jnp.bfloat16)
        for b in range(2):
            stage[pair, 2 * a + b] = result[:, 128 * b:128 * b + 128]
        send_out(pair, (2 * a, 2 * a + 1))

    none = jnp.full((8, rows), -jnp.inf, jnp.float32)
    zero = jnp.zeros((8, rows), jnp.float32)

    def turn_both(pair, a, peak, now, after):
        query = load_query(1 - a)
        top, total = none, zero
        for part in range(parts):
            top = score_part(query, after, part, top)
            total = weight_part(now, part, peak, total)
        finish(pair, a, total)
        return peak_of(top)

    def turn_last(pair, a, peak, now):
        total = zero
        for part in range(parts):
            total = weight_part(now, part, peak, total)
        finish(pair, a, total)

    @pl.when(owner)
    def _():
        pltpu.make_async_copy(kbuf, kbuf, k_sem.at[0]).wait()

        def flip(turn, carry):
            source = 2 * pair_of(lax.div(turn, 2)) + lax.rem(turn, 2)
            span = rows_of(source)
            pltpu.make_async_copy(vbuf.at[span], vbuf.at[span], v_sem.at[source]).wait()
            vflip[:, span] = vbuf[span, :].T
            return carry

        lax.fori_loop(0, peers, flip, 0)
        take_pair(pair_of(0))
        query = load_query(0)
        top = none
        for part in range(parts):
            top = score_part(query, sbuf0, part, top)

        def turns(at, peak):
            pair = pair_of(at)
            peak = turn_both(pair, 0, peak, sbuf0, sbuf1)
            take_pair(pair_of(at + 1))
            return turn_both(pair, 1, peak, sbuf1, sbuf0)

        peak = lax.fori_loop(0, peers // 2 - 1, turns, peak_of(top))
        last = pair_of(peers // 2 - 1)
        peak = turn_both(last, 0, peak, sbuf0, sbuf1)
        turn_last(last, 1, peak, sbuf1)

    pltpu.make_async_copy(out_ref, out_ref, out_recv.at[0]).wait()

    for kind in range(3):
        for step in range(peers - 1):
            @pl.when(heads[step] >= 0)
            def _():
                outgoing(kind, step).wait_send()

    @pl.when(owner)
    def _():
        pltpu.make_async_copy(stage, stage, out_send.at[0]).wait()


def on_device(queries, key_rows, value_rows):
    rows = queries.shape[0]
    total = rows * 16
    any_spec = pl.BlockSpec(memory_space=pl.ANY)
    flipped = pl.pallas_call(
        exchange,
        out_shape=jax.ShapeDtypeStruct((416, total // 4), jnp.bfloat16),
        in_specs=[any_spec] * 3,
        out_specs=pl.BlockSpec(memory_space=pl.ANY),
        scratch_shapes=[
            pltpu.VMEM((total, HEAD_DIM), jnp.bfloat16),
            pltpu.VMEM((total, HEAD_DIM), jnp.bfloat16),
            pltpu.VMEM((HEAD_DIM, total), jnp.bfloat16),
            pltpu.VMEM((total, HEAD_DIM), jnp.bfloat16),
            pltpu.VMEM((2 * rows, HEAD_DIM), jnp.float32),
            pltpu.VMEM((total, rows), jnp.float32),
            pltpu.VMEM((total, rows), jnp.float32),
            pltpu.VMEM((total, rows), jnp.bfloat16),
            pltpu.VMEM((8, 4, HEAD_DIM, HEAD_DIM), jnp.bfloat16),
            pltpu.SemaphoreType.DMA((3, 15)),
            pltpu.SemaphoreType.DMA((1,)),
            pltpu.SemaphoreType.DMA((16,)),
            pltpu.SemaphoreType.DMA((16,)),
            pltpu.SemaphoreType.DMA((1,)),
            pltpu.SemaphoreType.DMA((1,)),
        ],
        compiler_params=pltpu.CompilerParams(collective_id=0, has_side_effects=True, vmem_limit_bytes=VMEM_LIMIT),
    )(queries, key_rows, value_rows)
    return flipped.T


def solution(mesh):
    placed = (P(("dp", "seq"), None), P(("dp", "seq"), None), P(("dp", "seq"), None))
    return jax.shard_map(
        on_device, mesh=mesh, in_specs=placed, out_specs=P("dp", "seq"), check_vma=False
    )
```

```python
import functools
import math

import jax
import jax.numpy as jnp
from jax import lax
from jax.experimental import pallas as pl
from jax.experimental.pallas import tpu as pltpu
from jax.sharding import PartitionSpec as P

HEAD_DIM = 128
CHUNK = 512
VMEM_LIMIT = 60 * 1024 * 1024
MESH = pl.DeviceIdType.MESH
HEAD_AT = (
    (6, 10, 0, 3, 7, 11, 1, 4, 8, 12, -1, 5, 9, -1, 2, -1),
    (6, -1, 0, -1, 7, 10, -1, 3, 8, 11, 1, 4, 9, 12, 2, 5),
)
STEPS = ((0, 1), (1, 7), (0, 7), (1, 1), (0, 2), (1, 6), (0, 6), (1, 2),
         (0, 3), (1, 5), (0, 5), (1, 3), (0, 4), (1, 4), (1, 0))
PAIRS = ((0, 0), (1, 0), (0, 1), (1, 3), (0, 3), (1, 1), (0, 2), (1, 2))


def pick(table, index):
    value = jnp.int32(table[0])
    for place in range(1, len(table)):
        value = jnp.where(index == place, jnp.int32(table[place]), value)
    return value


def dot(a, b, dims):
    return lax.dot_general(a, b, (dims, ((), ())), preferred_element_type=jnp.float32)


def exchange(q_hbm, k_hbm, v_hbm, out_ref, kbuf, vbuf, vflip, qbuf, qwide, sbuf0, sbuf1, pbuf, stage,
             send_sem, k_sem, v_sem, q_sem, out_send, out_recv, ready):
    me = lax.axis_index("seq")
    core = lax.rem(lax.axis_index("dp"), 2)
    rows = q_hbm.shape[0]
    peers = 16
    tokens = rows * peers
    parts = tokens // CHUNK
    x_hi, z = lax.div(me, 8), lax.rem(me, 8)

    def place(dx, dz):
        return lax.rem(x_hi + dx, 2) * 8 + lax.rem(z + dz, 8)

    def head_at(where):
        return jnp.where(core == 0, pick(HEAD_AT[0], where), pick(HEAD_AT[1], where))

    my_head = head_at(me)
    owner = my_head >= 0

    barrier = pltpu.get_barrier_semaphore()
    for near in ((0, 1), (0, 7), (1, 0)):
        pl.semaphore_signal(barrier, inc=1, device_id={"seq": place(*near)}, device_id_type=MESH)

    targets = [place(dx, dz) for dx, dz in STEPS]
    heads = [head_at(target) for target in targets]

    def lanes_of(head):
        return pl.ds(pl.multiple_of(head * HEAD_DIM, HEAD_DIM), HEAD_DIM)

    def rows_of(source):
        return pl.ds(pl.multiple_of(source * rows, rows), rows)

    def outgoing(kind, step):
        src, dst = ((k_hbm, kbuf), (v_hbm, vbuf), (q_hbm, qbuf))[kind]
        sem = (k_sem.at[0], v_sem.at[me], q_sem.at[me])[kind]
        return pltpu.make_async_remote_copy(
            src_ref=src.at[:, lanes_of(heads[step])],
            dst_ref=dst.at[rows_of(me)],
            send_sem=send_sem.at[kind, step],
            recv_sem=sem,
            device_id={"seq": targets[step]},
            device_id_type=MESH,
        )

    def local(kind):
        src, dst = ((k_hbm, kbuf), (v_hbm, vbuf), (q_hbm, qbuf))[kind]
        sem = (k_sem.at[0], v_sem.at[me], q_sem.at[me])[kind]
        return pltpu.make_async_copy(src.at[:, lanes_of(my_head)], dst.at[rows_of(me)], sem)

    @pl.when(owner)
    def _():
        for kind in range(3):
            local(kind).start()

    def send(kind, step):
        @pl.when(heads[step] >= 0)
        def _():
            outgoing(kind, step).start()

    def keys_and_values(*offsets):
        for kind in range(2):
            for offset in offsets:
                send(kind, STEPS.index(offset))

    def tell(mark, dx, dz):
        pl.semaphore_signal(ready.at[mark], inc=1, device_id={"seq": place(dx, dz)}, device_id_type=MESH)

    def hear(*marks):
        for mark in marks:
            pl.semaphore_wait(ready.at[mark], 1)

    pl.semaphore_wait(barrier, 3)
    tell(0, 0, 1)
    tell(1, 0, 7)
    tell(5, 1, 0)
    keys_and_values((0, 1), (0, 7), (1, 0))
    hear(0, 1)
    tell(2, 0, 1)
    tell(3, 0, 7)
    tell(6, 1, 0)
    keys_and_values((0, 2), (0, 6))
    hear(5)
    keys_and_values((1, 7), (1, 1))
    hear(2, 3)
    tell(4, 0, 1)
    tell(7, 1, 0)
    keys_and_values((0, 3), (0, 5))
    hear(6)
    keys_and_values((1, 6), (1, 2))
    hear(4)
    tell(8, 1, 0)
    keys_and_values((0, 4))
    hear(7)
    keys_and_values((1, 5), (1, 3))
    hear(8)
    keys_and_values((1, 4))
    for step in range(peers - 1):
        send(2, step)

    first = my_head * 4
    low, high = lax.div(first, 13), lax.div(first + 3, 13)
    scale = math.log2(math.e) / math.sqrt(HEAD_DIM)

    def out_copy(pair, kind, group, unit, units):
        row = pl.multiple_of((first + unit - 13 * group) * 32, 32)
        return pltpu.make_async_remote_copy(
            src_ref=stage.at[pair, kind, pl.ds(32 * unit, 32 * units)],
            dst_ref=out_ref.at[pl.ds(row, 32 * units), pl.ds(pl.multiple_of(pair * 128, 128), 128)],
            send_sem=out_send.at[0],
            recv_sem=out_recv.at[0],
            device_id={"seq": 4 * kind + group},
            device_id_type=MESH,
        )

    def send_out(pair, kinds):
        @pl.when(high == low)
        def _():
            for kind in kinds:
                out_copy(pair, kind, low, 0, 4).start()

        @pl.when(high != low)
        def _():
            for kind in kinds:
                for unit in range(4):
                    out_copy(pair, kind, lax.div(first + unit, 13), unit, 1).start()

    def pair_of(turn):
        dx, dp = jnp.int32(0), jnp.int32(0)
        for at, (sx, sp) in enumerate(PAIRS):
            dx = jnp.where(turn == at, sx, dx)
            dp = jnp.where(turn == at, sp, dp)
        return lax.rem(x_hi + dx, 2) * 4 + lax.rem(lax.div(z, 2) + dp, 4)

    def fold(x, op):
        return op(x.reshape(x.shape[0] // 8, 8, x.shape[1]), axis=0)

    def take_pair(pair):
        for side in range(2):
            source = 2 * pair + side
            span = rows_of(source)
            pltpu.make_async_copy(qbuf.at[span], qbuf.at[span], q_sem.at[source]).wait()
            qwide[pl.ds(side * rows, rows), :] = qbuf[span, :].astype(jnp.float32)

    def load_query(a):
        picked = [
            qwide[pl.ds(rows * side + 128 * half + 64 * a + b, 32, stride=2), :]
            for b in range(2) for side in range(2) for half in range(2)
        ]
        return jnp.concatenate(picked, axis=0).astype(jnp.bfloat16)

    def score_part(query, scores, part, top):
        span = pl.ds(part * CHUNK, CHUNK)
        piece = dot(kbuf[span, :], query, ((1,), (1,)))
        scores[span, :] = piece
        return jnp.maximum(top, fold(piece, jnp.max))

    def weight_part(scores, part, peak, total):
        span = pl.ds(part * CHUNK, CHUNK)
        weights = jnp.exp2(scores[span, :] * scale - peak)
        pbuf[span, :] = weights.astype(jnp.bfloat16)
        return total + fold(weights, jnp.sum)

    def peak_of(top):
        return jnp.max(top, axis=0, keepdims=True) * scale

    def finish(pair, a, total):
        result = dot(vflip[...], pbuf[...], ((1,), (0,)))
        result = (result / jnp.sum(total, axis=0, keepdims=True)).astype(jnp.bfloat16)
        for b in range(2):
            stage[pair, 2 * a + b] = result[:, 128 * b:128 * b + 128]
        send_out(pair, (2 * a, 2 * a + 1))

    none = jnp.full((8, rows), -jnp.inf, jnp.float32)
    zero = jnp.zeros((8, rows), jnp.float32)

    def turn_both(pair, a, peak, now, after):
        query = load_query(1 - a)
        top, total = none, zero
        for part in range(parts):
            top = score_part(query, after, part, top)
            total = weight_part(now, part, peak, total)
        finish(pair, a, total)
        return peak_of(top)

    def turn_last(pair, a, peak, now):
        total = zero
        for part in range(parts):
            total = weight_part(now, part, peak, total)
        finish(pair, a, total)

    @pl.when(owner)
    def _():
        pltpu.make_async_copy(kbuf, kbuf, k_sem.at[0]).wait()

        def flip(turn, carry):
            source = 2 * pair_of(lax.div(turn, 2)) + lax.rem(turn, 2)
            span = rows_of(source)
            pltpu.make_async_copy(vbuf.at[span], vbuf.at[span], v_sem.at[source]).wait()
            vflip[:, span] = vbuf[span, :].T
            return carry

        lax.fori_loop(0, peers, flip, 0)
        take_pair(pair_of(0))
        query = load_query(0)
        top = none
        for part in range(parts):
            top = score_part(query, sbuf0, part, top)

        def turns(at, peak):
            pair = pair_of(at)
            peak = turn_both(pair, 0, peak, sbuf0, sbuf1)
            take_pair(pair_of(at + 1))
            return turn_both(pair, 1, peak, sbuf1, sbuf0)

        peak = lax.fori_loop(0, peers // 2 - 1, turns, peak_of(top))
        last = pair_of(peers // 2 - 1)
        peak = turn_both(last, 0, peak, sbuf0, sbuf1)
        turn_last(last, 1, peak, sbuf1)

    pltpu.make_async_copy(out_ref, out_ref, out_recv.at[0]).wait()

    for kind in range(3):
        for step in range(peers - 1):
            @pl.when(heads[step] >= 0)
            def _():
                outgoing(kind, step).wait_send()

    @pl.when(owner)
    def _():
        pltpu.make_async_copy(stage, stage, out_send.at[0]).wait()


def on_device(queries, key_rows, value_rows):
    rows = queries.shape[0]
    total = rows * 16
    any_spec = pl.BlockSpec(memory_space=pl.ANY)
    flipped = pl.pallas_call(
        exchange,
        out_shape=jax.ShapeDtypeStruct((416, total // 4), jnp.bfloat16),
        in_specs=[any_spec] * 3,
        out_specs=pl.BlockSpec(memory_space=pl.ANY),
        scratch_shapes=[
            pltpu.VMEM((total, HEAD_DIM), jnp.bfloat16),
            pltpu.VMEM((total, HEAD_DIM), jnp.bfloat16),
            pltpu.VMEM((HEAD_DIM, total), jnp.bfloat16),
            pltpu.VMEM((total, HEAD_DIM), jnp.bfloat16),
            pltpu.VMEM((2 * rows, HEAD_DIM), jnp.float32),
            pltpu.VMEM((total, rows), jnp.float32),
            pltpu.VMEM((total, rows), jnp.float32),
            pltpu.VMEM((total, rows), jnp.bfloat16),
            pltpu.VMEM((8, 4, HEAD_DIM, HEAD_DIM), jnp.bfloat16),
            pltpu.SemaphoreType.DMA((3, 15)),
            pltpu.SemaphoreType.DMA((1,)),
            pltpu.SemaphoreType.DMA((16,)),
            pltpu.SemaphoreType.DMA((16,)),
            pltpu.SemaphoreType.DMA((1,)),
            pltpu.SemaphoreType.DMA((1,)),
            pltpu.SemaphoreType.REGULAR((9,)),
        ],
        compiler_params=pltpu.CompilerParams(collective_id=0, has_side_effects=True, vmem_limit_bytes=VMEM_LIMIT),
    )(queries, key_rows, value_rows)
    return flipped.T


def solution(mesh):
    placed = (P(("dp", "seq"), None), P(("dp", "seq"), None), P(("dp", "seq"), None))
    return jax.shard_map(
        on_device, mesh=mesh, in_specs=placed, out_specs=P("dp", "seq"), check_vma=False
    )
```

```python
import functools
import math

import jax
import jax.numpy as jnp
from jax import lax
from jax.experimental import pallas as pl
from jax.experimental.pallas import tpu as pltpu
from jax.sharding import PartitionSpec as P

HEAD_DIM = 128
CHUNK = 512
VMEM_LIMIT = 60 * 1024 * 1024
MESH = pl.DeviceIdType.MESH
HEAD_AT = (
    (6, 10, 0, 3, 7, 11, 1, 4, 8, 12, -1, 5, 9, -1, 2, -1),
    (6, -1, 0, -1, 7, 10, -1, 3, 8, 11, 1, 4, 9, 12, 2, 5),
)
STEPS = ((0, 1), (1, 7), (0, 7), (1, 1), (0, 2), (1, 6), (0, 6), (1, 2),
         (0, 3), (1, 5), (0, 5), (1, 3), (0, 4), (1, 4), (1, 0))
PAIRS = ((0, 0), (1, 0), (0, 1), (1, 3), (0, 3), (1, 1), (0, 2), (1, 2))


def pick(table, index):
    value = jnp.int32(table[0])
    for place in range(1, len(table)):
        value = jnp.where(index == place, jnp.int32(table[place]), value)
    return value


def dot(a, b, dims):
    return lax.dot_general(a, b, (dims, ((), ())), preferred_element_type=jnp.float32)


def exchange(q_hbm, k_hbm, v_hbm, out_ref, kbuf, vbuf, vflip, qbuf, qwide, sbuf0, sbuf1, pbuf, stage,
             send_sem, k_sem, v_sem, q_sem, out_send, out_recv, ready):
    me = lax.axis_index("seq")
    core = lax.rem(lax.axis_index("dp"), 2)
    rows = q_hbm.shape[0]
    peers = 16
    tokens = rows * peers
    parts = tokens // CHUNK
    x_hi, z = lax.div(me, 8), lax.rem(me, 8)

    def place(dx, dz):
        return lax.rem(x_hi + dx, 2) * 8 + lax.rem(z + dz, 8)

    def head_at(where):
        return jnp.where(core == 0, pick(HEAD_AT[0], where), pick(HEAD_AT[1], where))

    my_head = head_at(me)
    owner = my_head >= 0

    barrier = pltpu.get_barrier_semaphore()
    for near in ((0, 1), (0, 7), (1, 0)):
        pl.semaphore_signal(barrier, inc=1, device_id={"seq": place(*near)}, device_id_type=MESH)

    targets = [place(dx, dz) for dx, dz in STEPS]
    heads = [head_at(target) for target in targets]

    def lanes_of(head):
        return pl.ds(pl.multiple_of(head * HEAD_DIM, HEAD_DIM), HEAD_DIM)

    def rows_of(source):
        return pl.ds(pl.multiple_of(source * rows, rows), rows)

    def outgoing(kind, step):
        src, dst = ((k_hbm, kbuf), (v_hbm, vbuf), (q_hbm, qbuf))[kind]
        sem = (k_sem.at[0], v_sem.at[me], q_sem.at[me])[kind]
        return pltpu.make_async_remote_copy(
            src_ref=src.at[:, lanes_of(heads[step])],
            dst_ref=dst.at[rows_of(me)],
            send_sem=send_sem.at[kind, step],
            recv_sem=sem,
            device_id={"seq": targets[step]},
            device_id_type=MESH,
        )

    def local(kind):
        src, dst = ((k_hbm, kbuf), (v_hbm, vbuf), (q_hbm, qbuf))[kind]
        sem = (k_sem.at[0], v_sem.at[me], q_sem.at[me])[kind]
        return pltpu.make_async_copy(src.at[:, lanes_of(my_head)], dst.at[rows_of(me)], sem)

    @pl.when(owner)
    def _():
        for kind in range(3):
            local(kind).start()

    def send(kind, step):
        @pl.when(heads[step] >= 0)
        def _():
            outgoing(kind, step).start()

    def keys_and_values(*offsets):
        for kind in range(2):
            for offset in offsets:
                send(kind, STEPS.index(offset))

    def tell(mark, dx, dz):
        pl.semaphore_signal(ready.at[mark], inc=1, device_id={"seq": place(dx, dz)}, device_id_type=MESH)

    def hear(*marks):
        for mark in marks:
            pl.semaphore_wait(ready.at[mark], 1)

    pl.semaphore_wait(barrier, 3)
    tell(0, 0, 1)
    tell(1, 0, 7)
    tell(5, 1, 0)
    keys_and_values((0, 1), (0, 7), (1, 0))
    hear(0, 1)
    tell(2, 0, 1)
    tell(3, 0, 7)
    tell(6, 1, 0)
    keys_and_values((0, 2), (0, 6))
    hear(5)
    keys_and_values((1, 7), (1, 1))
    hear(2, 3)
    tell(4, 0, 1)
    tell(7, 1, 0)
    keys_and_values((0, 3), (0, 5))
    hear(6)
    keys_and_values((1, 6), (1, 2))
    hear(4)
    tell(8, 1, 0)
    keys_and_values((0, 4))
    hear(7)
    keys_and_values((1, 5), (1, 3))
    hear(8)
    keys_and_values((1, 4))
    for step in range(peers - 1):
        send(2, step)

    first = my_head * 4
    low, high = lax.div(first, 13), lax.div(first + 3, 13)
    scale = math.log2(math.e) / math.sqrt(HEAD_DIM)

    def out_copy(pair, kind, group, unit, units):
        row = pl.multiple_of((first + unit - 13 * group) * 32, 32)
        return pltpu.make_async_remote_copy(
            src_ref=stage.at[pair, kind, pl.ds(32 * unit, 32 * units)],
            dst_ref=out_ref.at[pl.ds(row, 32 * units), pl.ds(pl.multiple_of(pair * 128, 128), 128)],
            send_sem=out_send.at[0],
            recv_sem=out_recv.at[0],
            device_id={"seq": 4 * kind + group},
            device_id_type=MESH,
        )

    def send_out(pair, kinds):
        @pl.when(high == low)
        def _():
            for kind in kinds:
                out_copy(pair, kind, low, 0, 4).start()

        @pl.when(high != low)
        def _():
            for kind in kinds:
                for unit in range(4):
                    out_copy(pair, kind, lax.div(first + unit, 13), unit, 1).start()

    def pair_of(turn):
        dx, dp = jnp.int32(0), jnp.int32(0)
        for at, (sx, sp) in enumerate(PAIRS):
            dx = jnp.where(turn == at, sx, dx)
            dp = jnp.where(turn == at, sp, dp)
        return lax.rem(x_hi + dx, 2) * 4 + lax.rem(lax.div(z, 2) + dp, 4)

    def fold(x, op):
        return op(x.reshape(x.shape[0] // 8, 8, x.shape[1]), axis=0)

    def take_pair(pair):
        for side in range(2):
            source = 2 * pair + side
            span = rows_of(source)
            pltpu.make_async_copy(qbuf.at[span], qbuf.at[span], q_sem.at[source]).wait()
            qwide[pl.ds(side * rows, rows), :] = qbuf[span, :].astype(jnp.float32)

    def load_query(b):
        picked = [
            qwide[pl.ds(rows * side + 128 * half + 64 * a + b, 32, stride=2), :]
            for a in range(2) for side in range(2) for half in range(2)
        ]
        return jnp.concatenate(picked, axis=0).astype(jnp.bfloat16)

    def score_part(query, scores, part, top):
        span = pl.ds(part * CHUNK, CHUNK)
        piece = dot(kbuf[span, :], query, ((1,), (1,)))
        scores[span, :] = piece
        return jnp.maximum(top, fold(piece, jnp.max))

    def weight_part(scores, part, peak, total):
        span = pl.ds(part * CHUNK, CHUNK)
        weights = jnp.exp2(scores[span, :] * scale - peak)
        pbuf[span, :] = weights.astype(jnp.bfloat16)
        return total + fold(weights, jnp.sum)

    def peak_of(top):
        return jnp.max(top, axis=0, keepdims=True) * scale

    def finish(pair, b, total):
        result = dot(vflip[...], pbuf[...], ((1,), (0,)))
        result = (result / jnp.sum(total, axis=0, keepdims=True)).astype(jnp.bfloat16)
        for a in range(2):
            stage[pair, 2 * a + b] = result[:, 128 * a:128 * a + 128]
        send_out(pair, (b, 2 + b))

    none = jnp.full((8, rows), -jnp.inf, jnp.float32)
    zero = jnp.zeros((8, rows), jnp.float32)

    def turn_both(pair, b, peak, now, after):
        query = load_query(1 - b)
        top, total = none, zero
        for part in range(parts):
            top = score_part(query, after, part, top)
            total = weight_part(now, part, peak, total)
        finish(pair, b, total)
        return peak_of(top)

    def turn_last(pair, b, peak, now):
        total = zero
        for part in range(parts):
            total = weight_part(now, part, peak, total)
        finish(pair, b, total)

    @pl.when(owner)
    def _():
        pltpu.make_async_copy(kbuf, kbuf, k_sem.at[0]).wait()

        def flip(turn, carry):
            source = 2 * pair_of(lax.div(turn, 2)) + lax.rem(turn, 2)
            span = rows_of(source)
            pltpu.make_async_copy(vbuf.at[span], vbuf.at[span], v_sem.at[source]).wait()
            vflip[:, span] = vbuf[span, :].T
            return carry

        lax.fori_loop(0, peers, flip, 0)
        take_pair(pair_of(0))
        query = load_query(0)
        top = none
        for part in range(parts):
            top = score_part(query, sbuf0, part, top)

        def turns(at, peak):
            pair = pair_of(at)
            peak = turn_both(pair, 0, peak, sbuf0, sbuf1)
            take_pair(pair_of(at + 1))
            return turn_both(pair, 1, peak, sbuf1, sbuf0)

        peak = lax.fori_loop(0, peers // 2 - 1, turns, peak_of(top))
        last = pair_of(peers // 2 - 1)
        peak = turn_both(last, 0, peak, sbuf0, sbuf1)
        turn_last(last, 1, peak, sbuf1)

    pltpu.make_async_copy(out_ref, out_ref, out_recv.at[0]).wait()

    for kind in range(3):
        for step in range(peers - 1):
            @pl.when(heads[step] >= 0)
            def _():
                outgoing(kind, step).wait_send()

    @pl.when(owner)
    def _():
        pltpu.make_async_copy(stage, stage, out_send.at[0]).wait()


def on_device(queries, key_rows, value_rows):
    rows = queries.shape[0]
    total = rows * 16
    any_spec = pl.BlockSpec(memory_space=pl.ANY)
    flipped = pl.pallas_call(
        exchange,
        out_shape=jax.ShapeDtypeStruct((416, total // 4), jnp.bfloat16),
        in_specs=[any_spec] * 3,
        out_specs=pl.BlockSpec(memory_space=pl.ANY),
        scratch_shapes=[
            pltpu.VMEM((total, HEAD_DIM), jnp.bfloat16),
            pltpu.VMEM((total, HEAD_DIM), jnp.bfloat16),
            pltpu.VMEM((HEAD_DIM, total), jnp.bfloat16),
            pltpu.VMEM((total, HEAD_DIM), jnp.bfloat16),
            pltpu.VMEM((2 * rows, HEAD_DIM), jnp.float32),
            pltpu.VMEM((total, rows), jnp.float32),
            pltpu.VMEM((total, rows), jnp.float32),
            pltpu.VMEM((total, rows), jnp.bfloat16),
            pltpu.VMEM((8, 4, HEAD_DIM, HEAD_DIM), jnp.bfloat16),
            pltpu.SemaphoreType.DMA((3, 15)),
            pltpu.SemaphoreType.DMA((1,)),
            pltpu.SemaphoreType.DMA((16,)),
            pltpu.SemaphoreType.DMA((16,)),
            pltpu.SemaphoreType.DMA((1,)),
            pltpu.SemaphoreType.DMA((1,)),
            pltpu.SemaphoreType.REGULAR((9,)),
        ],
        compiler_params=pltpu.CompilerParams(collective_id=0, has_side_effects=True, vmem_limit_bytes=VMEM_LIMIT),
    )(queries, key_rows, value_rows)
    return flipped.T


def solution(mesh):
    placed = (P(("dp", "seq"), None), P(("dp", "seq"), None), P(("dp", "seq"), None))
    return jax.shard_map(
        on_device, mesh=mesh, in_specs=placed, out_specs=P("dp", "seq"), check_vma=False
    )
```
